32 devices in a mesh: groups: 2 (over y), ep: 4 (over z), tok: 4 (over x, core).
Axes of the slice: x: 2, y: 2, z: 4, core: 2. Of those that a mesh axis runs over, the one named last changes fastest.
Arguments:
- tokens: bfloat16 [128, 7168], P(('groups', 'ep', 'tok')), parts along dimension 0, may hold values from -6 to 6
- expert_ids: int32 [128, 2], P(('groups', 'ep', 'tok')), parts along dimension 0, may hold values from 0 to 3, all different within a row; in each aligned block of 4 rows (0 to 3, 4 to 7, ...) at most 3 rows name the same one
- gate_fixed: int32 [128, 2], P(('groups', 'ep', 'tok')), parts along dimension 0, may hold values from 1 to 65535
- w_gate: bfloat16 [4, 7168, 2048], P('ep', None, 'tok'), may hold values from -0.0625 to 0.0625
- w_up: bfloat16 [4, 7168, 2048], P('ep', None, 'tok'), may hold values from -0.0625 to 0.0625
- w_down: bfloat16 [4, 2048, 7168], P('ep', 'tok'), may hold values from -0.125 to 0.125
Outputs:
- layer_out: bfloat16 [128, 7168], P(('groups', 'ep', 'tok')), parts along dimension 0
The draws below stay inside these ranges and needn't reach their ends.
There are 2 independent parts, one for each index of `groups`. The reference program is written for one: setup_inputs(seed, part) draws one part's arguments, and reference() takes and returns one part's arrays. A program takes and returns all parts, laid end to end along the dimension named above; an argument that names none is the same for every part. Nothing has to cross between parts.
Inputs may be any that keep to these rules, and one draw needn't show every extreme that they name: `expert_ids`: each row names 2 different experts. Among the 4 rows of one device no expert is named more than 3 times.
All inputs are finite; a program needn't handle non-finite values.
Results may differ from the reference program's by a relative error of at most 0.014.
Values may be sent and summed in bfloat16 or wider, within the bound.
A program may use at most 64 MiB of HBM per device.

```python
import math
import jax
import jax.numpy as jnp
import numpy as np
from jax import lax

D = 7168
FF = 2048
TOK_DEV = 4
EXPERTS = 4
TOPK = 2
MOST = 3
TOKENS = 64
N_TOK = 4


def touch_ends(drawn, key, smallest, top_value):
    longest = drawn.shape.index(max(drawn.shape))
    spots = []
    for shift in (0, 1):
        where = [jax.random.randint(jax.random.fold_in(key, axis), (), 0, length) for axis, length in enumerate(drawn.shape)]
        where[longest] = (where[longest] + shift) % drawn.shape[longest]
        spots.append(tuple(where))
    return drawn.at[spots[0]].set(smallest).at[spots[1]].set(top_value)


def level_of(own_key, shape, split, least, top_value):
    level, own = 1.0, jax.random.fold_in(own_key, 6)
    for axis_at, shards_of in split:
        draws = jnp.exp(jax.random.uniform(jax.random.fold_in(own, axis_at), (shards_of,), jnp.float32, least / len(split), top_value / len(split)))
        level = level * jnp.repeat(draws, shape[axis_at] // shards_of).reshape([-1 if axis == axis_at else 1 for axis in range(len(shape))])
    return level


def shared_out(own_key, own, number, rows, amount, top, most, lean):
    ranking = jax.random.permutation(own_key, amount)
    heavy_load, ordinary = load_shares(amount, rows * top, most, lean, True), load_shares(amount, rows * top, most, lean, False)
    places = jnp.arange(amount)

    def named(sizes, offset_by):
        used = int((sizes > 0).sum())
        fixed = max(1, used // 4)
        passed = fixed + (places - fixed + offset_by * (used - fixed)) % max(1, amount - fixed)
        return jnp.zeros((amount,), jnp.int32).at[ranking[jnp.where(places < fixed, places, passed)]].set(jnp.asarray(sizes, jnp.int32))

    sizes = jnp.where(number % 4 == 0, named(heavy_load, number // 4), named(ordinary, number - number // 4 - 1))
    mixed = jax.random.permutation(jax.random.fold_in(own, 3), amount)
    giver, receiver = mixed[0:amount // 2 * 2:2], mixed[1:amount // 2 * 2:2]
    room = jnp.minimum(sizes[giver] - 1, most - sizes[receiver]) // 2
    room = jnp.where((giver == ranking[0]) | (receiver == ranking[0]) | (sizes[receiver] == 0), 0, jnp.maximum(room, 0))
    passed = jax.random.randint(jax.random.fold_in(own, 4), (amount // 2,), 0, 1 << 20) % (room + 1)
    sizes = sizes.at[giver].add(-passed).at[receiver].add(passed)
    labels = jnp.searchsorted(jnp.cumsum(sizes), jnp.arange(rows * top), side="right").astype(jnp.int32)
    grid = labels.reshape(top, rows).T
    grid = grid[jax.random.permutation(jax.random.fold_in(own, 1), rows)]
    offset_by = jax.random.randint(jax.random.fold_in(own, 2), (rows, 1), 0, top)
    return jnp.take_along_axis(grid, (jnp.arange(top)[None, :] + offset_by) % top, axis=1)


def load_shares(amount, total, reach, slope, full):
    weights = [(1 << 20) // math.isqrt(grade ** slope) + 1 for grade in range(1, amount + 1)]
    largest = reach if full else min(reach, max(-(-total // amount), total * weights[0] // sum(weights)))
    least = 1 if total - largest >= amount - 1 else 0
    holding, spare = [largest] + [least] * (amount - 1), total - largest - least * (amount - 1)
    while spare > 0:
        candidates = [i for i in range(1, amount) if holding[i] < largest] or [i for i in range(1, amount) if holding[i] < reach]
        whole, left = sum([weights[i] for i in candidates]), spare
        for i in candidates:
            extra = min(reach - holding[i], max(1, left * weights[i] // whole), spare)
            holding[i] = holding[i] + extra
            spare = spare - extra
    return np.array(holding)


def scatter_about(own_key, extent, spread, limit, shards=(), kind=jnp.bfloat16):
    result = spread * jax.random.normal(own_key, extent, jnp.float32)
    if shards:
        result = result * level_of(own_key, extent, shards, -0.22, 0.18)
    return jnp.clip(result, -limit, limit).astype(kind)


def setup_inputs(seed: int = 0, part: int = 0) -> dict:
    seeds = jax.random.split(jax.random.key(seed), 7)
    part_splits = jax.random.split(jax.random.fold_in(seeds[6], part), 7)
    tokens = scatter_about(part_splits[0], (TOKENS, D), 1.0, 6.0, ((0, 16),))
    expert_ids_keys = jax.random.split(jax.random.fold_in(part_splits[1], 1), TOKENS // TOK_DEV)
    expert_ids_turns = jax.random.permutation(jax.random.fold_in(part_splits[1], 3), TOKENS // TOK_DEV)
    expert_ids = jax.vmap(lambda own, number: shared_out(jax.random.fold_in(part_splits[1], 2), own, number, TOK_DEV, EXPERTS, TOPK, MOST, 2))(expert_ids_keys, expert_ids_turns).reshape((TOKENS, TOPK))
    gate_fixed = touch_ends(jax.random.randint(part_splits[2], (TOKENS, TOPK), 1, 65536), jax.random.fold_in(part_splits[2], 1), 1, 65535).astype(jnp.int32)
    w_gate = scatter_about(seeds[3], (EXPERTS, D, FF), D ** -0.5, 0.0625, ((0, 4), (2, 4)))
    w_up = scatter_about(seeds[4], (EXPERTS, D, FF), D ** -0.5, 0.0625, ((0, 4), (2, 4)))
    w_down = scatter_about(seeds[5], (EXPERTS, FF, D), FF ** -0.5, 0.125, ((0, 4), (1, 4)))
    return dict(tokens=tokens, expert_ids=expert_ids, gate_fixed=gate_fixed, w_gate=w_gate, w_up=w_up, w_down=w_down)


def reference(tokens, expert_ids, gate_fixed, w_gate, w_up, w_down):
    scores = gate_fixed.astype(jnp.float32)
    weights = 2.5 * scores / jnp.sum(scores, axis=1, keepdims=True)
    slab_width = FF // N_TOK
    summed = jnp.zeros((TOKENS, D), jnp.float32)
    for expert in range(EXPERTS):
        gate = jnp.dot(tokens, w_gate[expert], preferred_element_type=jnp.float32)
        up_val = jnp.dot(tokens, w_up[expert], preferred_element_type=jnp.float32)
        hidden = (jax.nn.silu(gate) * up_val).astype(jnp.bfloat16)
        expert_out = jnp.zeros((TOKENS, D), jnp.float32)
        for slab in range(N_TOK):
            lower = slab * slab_width
            partial_value = jnp.dot(hidden[:, lower:lower + slab_width], w_down[expert, lower:lower + slab_width, :], preferred_element_type=jnp.float32)
            partial_value = lax.optimization_barrier(partial_value.astype(jnp.bfloat16)).astype(jnp.float32)
            expert_out = expert_out + partial_value
        weight_e = jnp.sum(weights * (expert_ids == expert).astype(jnp.float32), axis=1)
        summed = summed + weight_e[:, None] * expert_out
    return summed.astype(jnp.bfloat16)
```

```python
import functools

import jax
import jax.numpy as jnp
from jax import lax
from jax.experimental import pallas as pl
from jax.experimental.pallas import tpu as pltpu
from jax.sharding import PartitionSpec as P

MESH = pl.DeviceIdType.MESH
F32 = jnp.float32
BF16 = jnp.bfloat16


def chunks_of(width, wanted):
    for count in range(wanted, 0, -1):
        if width % (count * 128) == 0:
            return count
    return 1


def kernel(ep, cols, nk, nc, ids_ref, fixed_ref, tok_ref, wg_ref, wu_ref, wd_ref, out_ref,
           wg, wu, wd, tokbuf, wtbuf, xs, gacc, uacc, hid, part, r1, s1, r2, b3, r3,
           wg_sem, wu_sem, wd_sem, own_sem, sz, rz, sx, rx, sc, rc, s1s, r1s, s2s, r2s, s3s, r3s):
    e = lax.axis_index("ep")
    t = lax.axis_index("tok")
    x, c = t // 2, t % 2
    q = c * cols + x
    rows = tok_ref.shape[0]
    kc, nw = tokbuf.shape[-1], part.shape[-1]
    half = part.shape[1] // 2
    block = half // cols

    own = [pltpu.make_async_copy(tok_ref.at[:, pl.ds(k * kc, kc)], tokbuf.at[k, q, e], own_sem.at[k]) for k in range(nk)]
    for cp in own:
        cp.start()
    gcp = [pltpu.make_async_copy(wg_ref.at[0, pl.ds(k * kc, kc), :], wg.at[k], wg_sem.at[k]) for k in range(nk)]
    ucp = [pltpu.make_async_copy(wu_ref.at[0, pl.ds(k * kc, kc), :], wu.at[k], wu_sem.at[k]) for k in range(nk)]
    dcp = [pltpu.make_async_copy(wd_ref.at[0, :, pl.ds(n * nw, nw)], wd.at[n], wd_sem.at[n]) for n in range(nc)]
    for k in range(nk):
        gcp[k].start()
        ucp[k].start()
    for n in range(nc):
        dcp[n].start()

    scores = fixed_ref[...].astype(F32)
    weights = 2.5 * scores / jnp.sum(scores, axis=1, keepdims=True)
    ids = ids_ref[...]
    lane = lax.broadcasted_iota(jnp.int32, (rows, 128), 1)
    table = jnp.zeros((rows, 128), F32)
    for j in range(ids.shape[1]):
        table = table + jnp.where(lane == ids[:, j:j + 1], weights[:, j:j + 1], 0.0)
    wtbuf[q, e] = table

    def at_z(d):
        return {"ep": lax.rem(e + d, ep)}

    def at_x(d):
        return {"tok": lax.rem(x + d, cols) * 2 + c}

    partner = {"tok": x * 2 + 1 - c}
    barrier = pltpu.get_barrier_semaphore()
    for d in range(1, ep):
        pl.semaphore_signal(barrier, inc=1, device_id=at_z(d), device_id_type=MESH)
    for d in range(1, cols):
        pl.semaphore_signal(barrier, inc=1, device_id=at_x(d), device_id_type=MESH)
    pl.semaphore_signal(barrier, inc=1, device_id=partner, device_id_type=MESH)
    pl.semaphore_wait(barrier, ep - 1 + cols - 1 + 1)

    sends = []

    def send(src, dst, ssem, rsem, to):
        cp = pltpu.make_async_remote_copy(src_ref=src, dst_ref=dst, send_sem=ssem, recv_sem=rsem, device_id=to, device_id_type=MESH)
        cp.start()
        sends.append(cp)

    def took(ref, sem):
        pltpu.make_async_copy(ref, ref, sem).wait()

    def buf(k):
        return tokbuf.at[k] if k < nk else wtbuf

    def forward_x(k, d_src, src):
        b = buf(k).at[q, src]
        for d in range(1, cols):
            send(b, b, sx.at[k, d_src, d - 1], rx.at[k, d - 1], at_x(d))

    def begin(k):
        if k < nk:
            own[k].wait()
        b = buf(k).at[q, e]
        for d in range(1, ep):
            send(b, b, sz.at[k, d - 1], rz.at[k, d - 1], at_z(d))
        forward_x(k, 0, e)

    def z_stage(k):
        for d in range(1, ep):
            src = lax.rem(e + ep - d, ep)
            took(buf(k).at[q, src], rz.at[k, d - 1])
            forward_x(k, d, src)
        b = buf(k).at[q]
        send(b, b, sc.at[k, 0], rc.at[k], partner)

    def x_stage(k):
        for d in range(1, cols):
            p = c * cols + lax.rem(x + cols - d, cols)
            b = buf(k).at[p]
            took(b, rx.at[k, d - 1])
            send(b, b, sc.at[k, d], rc.at[k], partner)

    def c_stage(k):
        took(buf(k).at[pl.ds((1 - c) * cols, cols)], rc.at[k])

    group = max(1, 16 // rows)

    def matmuls(k):
        for p in range(2 * cols):
            for g in range(0, ep, group):
                span = min(group, ep - g)
                piece = jnp.concatenate([tokbuf[k, p, g + i].astype(F32) for i in range(span)], axis=0).astype(BF16)
                xs[pl.ds((p * ep + g) * rows, span * rows), :] = piece
        gcp[k].wait()
        gate = jnp.dot(xs[...], wg[k], preferred_element_type=F32)
        if k == 0:
            gacc[...] = gate
        else:
            gacc[...] += gate
        ucp[k].wait()
        up = jnp.dot(xs[...], wu[k], preferred_element_type=F32)
        if k == 0:
            uacc[...] = up
        else:
            uacc[...] += up

    order = list(range(nk))
    for k in range(nk + 1):
        begin(k)
    for s in range(nk + 3):
        if s <= nk:
            z_stage(s)
        if 0 <= s - 1 <= nk:
            x_stage(s - 1)
        if 0 <= s - 2 <= nk:
            c_stage(s - 2)
            if s - 2 < nk:
                matmuls(s - 2)

    tab = jnp.concatenate([wtbuf[p, i] for p in range(2 * cols) for i in range(ep)], axis=0)
    lanes = lax.broadcasted_iota(jnp.int32, tab.shape, 1)
    scale = jnp.sum(jnp.where(lanes == e, tab, 0.0), axis=1, keepdims=True)
    gate = gacc[...]
    hid[...] = (gate / (1.0 + jnp.exp(-gate)) * uacc[...] * scale).astype(BF16)

    def down(n):
        dcp[n].wait()
        part[n] = jnp.dot(hid[...], wd[n], preferred_element_type=F32).astype(BF16)
        send(part.at[n, pl.ds((1 - c) * half, half)], r1.at[n], s1s.at[n], r1s.at[n], partner)

    def sum_core(n):
        took(r1.at[n], r1s.at[n])
        mine = part[n, pl.ds(c * half, half), :].astype(F32) + r1[n].astype(F32)
        s1[n] = mine.astype(BF16)
        for d in range(1, cols):
            to = lax.rem(x + d, cols)
            send(s1.at[n, pl.ds(to * block, block)], r2.at[n, d - 1], s2s.at[n, d - 1], r2s.at[n], at_x(d))

    def sum_x(n):
        took(r2.at[n], r2s.at[n])
        mine = s1[n, pl.ds(x * block, block), :].astype(F32)
        for d in range(cols - 1):
            mine = mine + r2[n, d].astype(F32)
        for i in range(ep):
            b3[n, i] = mine[i * rows:(i + 1) * rows].astype(BF16)
        for d in range(1, ep):
            to = lax.rem(e + d, ep)
            send(b3.at[n, to], r3.at[n, d - 1], s3s.at[n, d - 1], r3s.at[n], at_z(d))

    def sum_z(n):
        took(r3.at[n], r3s.at[n])
        total = b3[n, e].astype(F32)
        for d in range(ep - 1):
            total = total + r3[n, d].astype(F32)
        out_ref[:, n * nw:(n + 1) * nw] = total.astype(BF16)

    for s in range(nc + 3):
        if s < nc:
            down(s)
        if 0 <= s - 1 < nc:
            sum_core(s - 1)
        if 0 <= s - 2 < nc:
            sum_x(s - 2)
        if 0 <= s - 3 < nc:
            sum_z(s - 3)
    for cp in sends:
        cp.wait_send()


def solution(mesh):
    ep, tok = mesh.shape["ep"], mesh.shape["tok"]
    cols = tok // 2

    def step(tokens, expert_ids, gate_fixed, w_gate, w_up, w_down):
        rows, width = tokens.shape
        ff = w_gate.shape[2]
        m = ep * tok * rows
        nk = chunks_of(width, 4)
        nc = chunks_of(width, 4)
        kc, nw = width // nk, width // nc
        dma = pltpu.SemaphoreType.DMA
        vmem = pl.BlockSpec(memory_space=pltpu.VMEM)
        anywhere = pl.BlockSpec(memory_space=pl.ANY)
        return pl.pallas_call(
            functools.partial(kernel, ep, cols, nk, nc),
            out_shape=jax.ShapeDtypeStruct((rows, width), BF16),
            in_specs=[vmem, vmem, anywhere, anywhere, anywhere, anywhere],
            out_specs=vmem,
            scratch_shapes=[
                pltpu.VMEM((nk, kc, ff), BF16),
                pltpu.VMEM((nk, kc, ff), BF16),
                pltpu.VMEM((nc, ff, nw), BF16),
                pltpu.VMEM((nk, tok, ep, rows, kc), BF16),
                pltpu.VMEM((tok, ep, rows, 128), F32),
                pltpu.VMEM((m, kc), BF16),
                pltpu.VMEM((m, ff), F32),
                pltpu.VMEM((m, ff), F32),
                pltpu.VMEM((m, ff), BF16),
                pltpu.VMEM((nc, m, nw), BF16),
                pltpu.VMEM((nc, m // 2, nw), BF16),
                pltpu.VMEM((nc, m // 2, nw), BF16),
                pltpu.VMEM((nc, cols - 1, ep * rows, nw), BF16),
                pltpu.VMEM((nc, ep, rows, nw), BF16),
                pltpu.VMEM((nc, ep - 1, rows, nw), BF16),
                dma((nk,)), dma((nk,)), dma((nc,)), dma((nk,)),
                dma((nk + 1, ep - 1)), dma((nk + 1, ep - 1)),
                dma((nk + 1, ep, cols - 1)), dma((nk + 1, cols - 1)),
                dma((nk + 1, cols)), dma((nk + 1,)),
                dma((nc,)), dma((nc,)),
                dma((nc, cols - 1)), dma((nc,)),
                dma((nc, ep - 1)), dma((nc,)),
            ],
            compiler_params=pltpu.CompilerParams(
                collective_id=0, has_side_effects=True, vmem_limit_bytes=64000000,
            ),
        )(expert_ids, gate_fixed, tokens, w_gate, w_up, w_down)

    rows_spec = P(("groups", "ep", "tok"), None)
    return jax.shard_map(
        step, mesh=mesh,
        in_specs=(rows_spec, rows_spec, rows_spec, P("ep", None, "tok"), P("ep", None, "tok"), P("ep", "tok", None)),
        out_specs=rows_spec, check_vma=False,
    )
```

```python
import functools

import jax
import jax.numpy as jnp
from jax import lax
from jax.experimental import pallas as pl
from jax.experimental.pallas import tpu as pltpu
from jax.sharding import PartitionSpec as P

MESH = pl.DeviceIdType.MESH
F32 = jnp.float32
BF16 = jnp.bfloat16
NK, NC = 2, 4
AGX, AGC = 1, 1
LAG1, LAG2, LAG3 = 1, 3, 3


def chunks_of(width, wanted):
    for count in range(wanted, 0, -1):
        if width % (count * 128) == 0:
            return count
    return 1


def paired(v, d):
    bit = 1
    while bit <= d:
        if d & bit:
            v = v + bit - 2 * bit * (lax.rem(v // bit, 2))
        bit *= 2
    return v


def kernel(ep, cols, nk, nc, ids_hbm, fixed_hbm, tok_ref, wg_ref, wu_ref, wd_ref, out_ref,
           ids_ref, fixed_ref, wg, wu, wd, tokbuf, wtbuf, xs, gacc, uacc, hid, part, r1, s1, r2, b3, r3,
           id_sem, wg_sem, wu_sem, wd_sem, own_sem, sz, rz, sx, rx, sc, rc, s1s, r1s, s2s, r2s, s3s, r3s):
    e = lax.axis_index("ep")
    t = lax.axis_index("tok")
    x, c = t // 2, t % 2
    q = c * cols + x
    rows = tok_ref.shape[0]
    kc, nw = tokbuf.shape[-1], part.shape[-1]
    half = part.shape[1] // 2
    block = half // cols

    idcp = [pltpu.make_async_copy(a, b, id_sem.at[i]) for i, (a, b) in enumerate(((ids_hbm, ids_ref), (fixed_hbm, fixed_ref)))]
    for cp in idcp:
        cp.start()
    own = [pltpu.make_async_copy(tok_ref.at[:, pl.ds(k * kc, kc)], tokbuf.at[k, q, e], own_sem.at[k]) for k in range(nk)]
    for cp in own:
        cp.start()
    gcp = [pltpu.make_async_copy(wg_ref.at[0, pl.ds(k * kc, kc), :], wg.at[k], wg_sem.at[k]) for k in range(nk)]
    ucp = [pltpu.make_async_copy(wu_ref.at[0, pl.ds(k * kc, kc), :], wu.at[k], wu_sem.at[k]) for k in range(nk)]
    dcp = [pltpu.make_async_copy(wd_ref.at[0, :, pl.ds(n * nw, nw)], wd.at[n], wd_sem.at[n]) for n in range(nc)]
    for k in range(nk):
        gcp[k].start()
        ucp[k].start()
    for n in range(nc):
        dcp[n].start()

    def at_z(d):
        return {"ep": paired(e, d)}

    def at_x(d):
        return {"tok": lax.rem(x + d, cols) * 2 + c}

    partner = {"tok": x * 2 + 1 - c}
    barrier = pltpu.get_barrier_semaphore()
    for d in range(1, ep):
        pl.semaphore_signal(barrier, inc=1, device_id=at_z(d), device_id_type=MESH)
    for d in range(1, cols):
        pl.semaphore_signal(barrier, inc=1, device_id=at_x(d), device_id_type=MESH)
    pl.semaphore_signal(barrier, inc=1, device_id=partner, device_id_type=MESH)
    for cp in idcp:
        cp.wait()
    scores = fixed_ref[...].astype(F32)
    weights = 2.5 * scores / jnp.sum(scores, axis=0, keepdims=True)
    ids = ids_ref[...].astype(F32)
    lane = lax.broadcasted_iota(jnp.int32, (rows, 128), 1).astype(F32)
    eye = lax.broadcasted_iota(jnp.int32, (rows, rows), 0) == lax.broadcasted_iota(jnp.int32, (rows, rows), 1)

    def column(row):
        return jnp.sum(jnp.where(eye, jnp.broadcast_to(row, (rows, rows)), 0.0), axis=1, keepdims=True)

    table = jnp.zeros((rows, 128), F32)
    for j in range(ids.shape[0]):
        table = table + jnp.where(lane == column(ids[j:j + 1]), column(weights[j:j + 1]), 0.0)
    wtbuf[q, e] = table
    pl.semaphore_wait(barrier, ep - 1 + cols - 1 + 1)

    sends = []

    def send(src, dst, ssem, rsem, to):
        cp = pltpu.make_async_remote_copy(src_ref=src, dst_ref=dst, send_sem=ssem, recv_sem=rsem, device_id=to, device_id_type=MESH)
        cp.start()
        sends.append(cp)

    def took(ref, sem):
        pltpu.make_async_copy(ref, ref, sem).wait()

    def buf(k):
        return tokbuf.at[k] if k < nk else wtbuf

    def forward_x(k, d_src, src):
        b = buf(k).at[q, src]
        for d in range(1, cols):
            send(b, b, sx.at[k, d_src, d - 1], rx.at[k, d - 1], at_x(d))

    def begin(k):
        if k < nk:
            own[k].wait()
        b = buf(k).at[q, e]
        for d in range(1, ep):
            send(b, b, sz.at[k, d - 1], rz.at[k, d - 1], at_z(d))
        forward_x(k, 0, e)

    def z_stage(k):
        for d in range(1, ep):
            src = paired(e, d)
            took(buf(k).at[q, src], rz.at[k, d - 1])
            forward_x(k, d, src)
        b = buf(k).at[q]
        send(b, b, sc.at[k, 0], rc.at[k], partner)

    def x_stage(k):
        for d in range(1, cols):
            p = c * cols + lax.rem(x + cols - d, cols)
            b = buf(k).at[p]
            took(b, rx.at[k, d - 1])
            send(b, b, sc.at[k, d], rc.at[k], partner)

    def c_stage(k):
        took(buf(k).at[pl.ds((1 - c) * cols, cols)], rc.at[k])

    group = max(1, 16 // rows)

    def matmuls(k):
        for p in range(2 * cols):
            for g in range(0, ep, group):
                span = min(group, ep - g)
                piece = jnp.concatenate([tokbuf[k, p, g + i].astype(F32) for i in range(span)], axis=0).astype(BF16)
                xs[pl.ds((p * ep + g) * rows, span * rows), :] = piece
        gcp[k].wait()
        gate = jnp.dot(xs[...], wg[k], preferred_element_type=F32)
        if k == 0:
            gacc[...] = gate
        else:
            gacc[...] += gate
        ucp[k].wait()
        up = jnp.dot(xs[...], wu[k], preferred_element_type=F32)
        if k == 0:
            uacc[...] = up
        else:
            uacc[...] += up

    for k in range(nk + 1):
        begin(k)
    for s in range(nk + 1 + AGX + AGC):
        if s <= nk:
            z_stage(s)
        if 0 <= s - AGX <= nk:
            x_stage(s - AGX)
        if 0 <= s - AGX - AGC <= nk:
            c_stage(s - AGX - AGC)
            if s - AGX - AGC < nk:
                matmuls(s - AGX - AGC)

    tab = jnp.concatenate([wtbuf[p, i] for p in range(2 * cols) for i in range(ep)], axis=0)
    lanes = lax.broadcasted_iota(jnp.int32, tab.shape, 1)
    scale = jnp.sum(jnp.where(lanes == e, tab, 0.0), axis=1, keepdims=True)
    gate = gacc[...]
    hid[...] = (gate / (1.0 + jnp.exp(-gate)) * uacc[...] * scale).astype(BF16)

    def down(n):
        dcp[n].wait()
        part[n] = jnp.dot(hid[...], wd[n], preferred_element_type=F32).astype(BF16)
        send(part.at[n, pl.ds((1 - c) * half, half)], r1.at[n], s1s.at[n], r1s.at[n], partner)

    def sum_core(n):
        took(r1.at[n], r1s.at[n])
        mine = part[n, pl.ds(c * half, half), :].astype(F32) + r1[n].astype(F32)
        s1[n] = mine.astype(BF16)
        for d in range(1, cols):
            to = lax.rem(x + d, cols)
            send(s1.at[n, pl.ds(to * block, block)], r2.at[n, d - 1], s2s.at[n, d - 1], r2s.at[n], at_x(d))

    def sum_x(n):
        took(r2.at[n], r2s.at[n])
        mine = s1[n, pl.ds(x * block, block), :].astype(F32)
        for d in range(cols - 1):
            mine = mine + r2[n, d].astype(F32)
        for i in range(ep):
            b3[n, i] = mine[i * rows:(i + 1) * rows].astype(BF16)
        for d in range(1, ep):
            to = paired(e, d)
            send(b3.at[n, to], r3.at[n, d - 1], s3s.at[n, d - 1], r3s.at[n], at_z(d))

    def sum_z(n):
        took(r3.at[n], r3s.at[n])
        total = b3[n, e].astype(F32)
        for d in range(ep - 1):
            total = total + r3[n, d].astype(F32)
        out_ref[:, n * nw:(n + 1) * nw] = total.astype(BF16)

    for s in range(nc + LAG1 + LAG2 + LAG3):
        if s < nc:
            down(s)
        if 0 <= s - LAG1 < nc:
            sum_core(s - LAG1)
        if 0 <= s - LAG1 - LAG2 < nc:
            sum_x(s - LAG1 - LAG2)
        if 0 <= s - LAG1 - LAG2 - LAG3 < nc:
            sum_z(s - LAG1 - LAG2 - LAG3)
    for cp in sends:
        cp.wait_send()


def solution(mesh):
    ep, tok = mesh.shape["ep"], mesh.shape["tok"]
    cols = tok // 2

    def step(tokens, expert_ids, gate_fixed, w_gate, w_up, w_down):
        rows, width = tokens.shape
        ff = w_gate.shape[2]
        m = ep * tok * rows
        nk = chunks_of(width, NK)
        nc = chunks_of(width, NC)
        kc, nw = width // nk, width // nc
        dma = pltpu.SemaphoreType.DMA
        vmem = pl.BlockSpec(memory_space=pltpu.VMEM)
        anywhere = pl.BlockSpec(memory_space=pl.ANY)
        return pl.pallas_call(
            functools.partial(kernel, ep, cols, nk, nc),
            out_shape=jax.ShapeDtypeStruct((rows, width), BF16),
            in_specs=[anywhere, anywhere, anywhere, anywhere, anywhere, anywhere],
            out_specs=vmem,
            scratch_shapes=[
                pltpu.VMEM(expert_ids.shape[::-1], jnp.int32),
                pltpu.VMEM(gate_fixed.shape[::-1], jnp.int32),
                pltpu.VMEM((nk, kc, ff), BF16),
                pltpu.VMEM((nk, kc, ff), BF16),
                pltpu.VMEM((nc, ff, nw), BF16),
                pltpu.VMEM((nk, tok, ep, rows, kc), BF16),
                pltpu.VMEM((tok, ep, rows, 128), F32),
                pltpu.VMEM((m, kc), BF16),
                pltpu.VMEM((m, ff), F32),
                pltpu.VMEM((m, ff), F32),
                pltpu.VMEM((m, ff), BF16),
                pltpu.VMEM((nc, m, nw), BF16),
                pltpu.VMEM((nc, m // 2, nw), BF16),
                pltpu.VMEM((nc, m // 2, nw), BF16),
                pltpu.VMEM((nc, cols - 1, ep * rows, nw), BF16),
                pltpu.VMEM((nc, ep, rows, nw), BF16),
                pltpu.VMEM((nc, ep - 1, rows, nw), BF16),
                dma((2,)), dma((nk,)), dma((nk,)), dma((nc,)), dma((nk,)),
                dma((nk + 1, ep - 1)), dma((nk + 1, ep - 1)),
                dma((nk + 1, ep, cols - 1)), dma((nk + 1, cols - 1)),
                dma((nk + 1, cols)), dma((nk + 1,)),
                dma((nc,)), dma((nc,)),
                dma((nc, cols - 1)), dma((nc,)),
                dma((nc, ep - 1)), dma((nc,)),
            ],
            compiler_params=pltpu.CompilerParams(
                collective_id=0, has_side_effects=True, vmem_limit_bytes=64000000,
            ),
        )(expert_ids.T, gate_fixed.T, tokens, w_gate, w_up, w_down)

    rows_spec = P(("groups", "ep", "tok"), None)
    return jax.shard_map(
        step, mesh=mesh,
        in_specs=(rows_spec, rows_spec, rows_spec, P("ep", None, "tok"), P("ep", None, "tok"), P("ep", "tok", None)),
        out_specs=rows_spec, check_vma=False,
    )
```

```python
import functools

import jax
import jax.numpy as jnp
from jax import lax
from jax.experimental import pallas as pl
from jax.experimental.pallas import tpu as pltpu
from jax.sharding import PartitionSpec as P

MESH = pl.DeviceIdType.MESH
F32 = jnp.float32
BF16 = jnp.bfloat16
NK, NC = 2, 4
AGX, AGC = 2, 1
LAG1, LAG2, LAG3 = 1, 3, 3


def chunks_of(width, wanted):
    for count in range(wanted, 0, -1):
        if width % (count * 128) == 0:
            return count
    return 1


def paired(v, d):
    bit = 1
    while bit <= d:
        if d & bit:
            v = v + bit - 2 * bit * (lax.rem(v // bit, 2))
        bit *= 2
    return v


def kernel(ep, cols, nk, nc, ids_hbm, fixed_hbm, tok_ref, wg_ref, wu_ref, wd_ref, out_ref,
           ids_ref, fixed_ref, wg, wu, wd, tokbuf, wtbuf, xs, gacc, uacc, hid, part, r1, s1, r2, b3, r3,
           id_sem, wg_sem, wu_sem, wd_sem, own_sem, sz, rz, sx, rx, sc, rc, s1s, r1s, s2s, r2s, s3s, r3s):
    e = lax.axis_index("ep")
    t = lax.axis_index("tok")
    x, c = t // 2, t % 2
    q = c * cols + x
    rows = tok_ref.shape[0]
    kc, nw = tokbuf.shape[-1], part.shape[-1]
    half = part.shape[1] // 2
    block = half // cols

    idcp = [pltpu.make_async_copy(a, b, id_sem.at[i]) for i, (a, b) in enumerate(((ids_hbm, ids_ref), (fixed_hbm, fixed_ref)))]
    for cp in idcp:
        cp.start()
    own = [pltpu.make_async_copy(tok_ref.at[:, pl.ds(k * kc, kc)], tokbuf.at[k, q, e], own_sem.at[k]) for k in range(nk)]
    for cp in own:
        cp.start()
    gcp = [pltpu.make_async_copy(wg_ref.at[0, pl.ds(k * kc, kc), :], wg.at[k], wg_sem.at[k]) for k in range(nk)]
    ucp = [pltpu.make_async_copy(wu_ref.at[0, pl.ds(k * kc, kc), :], wu.at[k], wu_sem.at[k]) for k in range(nk)]
    dcp = [pltpu.make_async_copy(wd_ref.at[0, :, pl.ds(n * nw, nw)], wd.at[n], wd_sem.at[n]) for n in range(nc)]
    for k in range(nk):
        gcp[k].start()
        ucp[k].start()
    for n in range(nc):
        dcp[n].start()

    def at_z(d):
        return {"ep": paired(e, d)}

    def at_x(d):
        return {"tok": lax.rem(x + d, cols) * 2 + c}

    partner = {"tok": x * 2 + 1 - c}
    barrier = pltpu.get_barrier_semaphore()
    for d in range(1, ep):
        pl.semaphore_signal(barrier, inc=1, device_id=at_z(d), device_id_type=MESH)
    for d in range(1, cols):
        pl.semaphore_signal(barrier, inc=1, device_id=at_x(d), device_id_type=MESH)
    pl.semaphore_signal(barrier, inc=1, device_id=partner, device_id_type=MESH)
    for cp in idcp:
        cp.wait()
    scores = fixed_ref[...].astype(F32)
    weights = 2.5 * scores / jnp.sum(scores, axis=0, keepdims=True)
    ids = ids_ref[...].astype(F32)
    lane = lax.broadcasted_iota(jnp.int32, (rows, 128), 1).astype(F32)
    eye = lax.broadcasted_iota(jnp.int32, (rows, rows), 0) == lax.broadcasted_iota(jnp.int32, (rows, rows), 1)

    def column(row):
        return jnp.sum(jnp.where(eye, jnp.broadcast_to(row, (rows, rows)), 0.0), axis=1, keepdims=True)

    table = jnp.zeros((rows, 128), F32)
    for j in range(ids.shape[0]):
        table = table + jnp.where(lane == column(ids[j:j + 1]), column(weights[j:j + 1]), 0.0)
    wtbuf[q, e] = table
    pl.semaphore_wait(barrier, ep - 1 + cols - 1 + 1)

    sends = []

    def send(src, dst, ssem, rsem, to):
        cp = pltpu.make_async_remote_copy(src_ref=src, dst_ref=dst, send_sem=ssem, recv_sem=rsem, device_id=to, device_id_type=MESH)
        cp.start()
        sends.append(cp)

    def took(ref, sem):
        pltpu.make_async_copy(ref, ref, sem).wait()

    def buf(k):
        return tokbuf.at[k] if k < nk else wtbuf

    def forward_x(k, d_src, src):
        b = buf(k).at[q, src]
        for d in range(1, cols):
            send(b, b, sx.at[k, d_src, d - 1], rx.at[k, d - 1], at_x(d))

    def begin(k):
        if k < nk:
            own[k].wait()
        b = buf(k).at[q, e]
        for d in range(1, ep):
            send(b, b, sz.at[k, d - 1], rz.at[k, d - 1], at_z(d))
        forward_x(k, 0, e)

    def z_stage(k):
        for d in range(1, ep):
            src = paired(e, d)
            took(buf(k).at[q, src], rz.at[k, d - 1])
            forward_x(k, d, src)
        b = buf(k).at[q]
        send(b, b, sc.at[k, 0], rc.at[k], partner)

    def x_stage(k):
        for d in range(1, cols):
            p = c * cols + lax.rem(x + cols - d, cols)
            b = buf(k).at[p]
            took(b, rx.at[k, d - 1])
            send(b, b, sc.at[k, d], rc.at[k], partner)

    def c_stage(k):
        took(buf(k).at[pl.ds((1 - c) * cols, cols)], rc.at[k])

    group = max(1, 16 // rows)

    def matmuls(k):
        for i_p in range(2 * cols):
            if i_p == cols:
                c_stage(k)
            p = (c if i_p < cols else 1 - c) * cols + i_p % cols
            for g in range(0, ep, group):
                span = min(group, ep - g)
                piece = jnp.concatenate([tokbuf[k, p, g + i].astype(F32) for i in range(span)], axis=0).astype(BF16)
                xs[pl.ds(pl.multiple_of((p * ep + g) * rows, span * rows), span * rows), :] = piece
        gcp[k].wait()
        gate = jnp.dot(xs[...], wg[k], preferred_element_type=F32)
        if k == 0:
            gacc[...] = gate
        else:
            gacc[...] += gate
        ucp[k].wait()
        up = jnp.dot(xs[...], wu[k], preferred_element_type=F32)
        if k == 0:
            uacc[...] = up
        else:
            uacc[...] += up

    for k in range(nk + 1):
        begin(k)
    for s in range(nk + 1 + AGX + AGC):
        if s <= nk:
            z_stage(s)
        if 0 <= s - AGX <= nk:
            x_stage(s - AGX)
        if 0 <= s - AGX - AGC <= nk:
            if s - AGX - AGC < nk:
                matmuls(s - AGX - AGC)
            else:
                c_stage(nk)

    tab = jnp.concatenate([wtbuf[p, i] for p in range(2 * cols) for i in range(ep)], axis=0)
    lanes = lax.broadcasted_iota(jnp.int32, tab.shape, 1)
    scale = jnp.sum(jnp.where(lanes == e, tab, 0.0), axis=1, keepdims=True)
    gate = gacc[...]
    hid[...] = (gate / (1.0 + jnp.exp(-gate)) * uacc[...] * scale).astype(BF16)

    def down(n):
        dcp[n].wait()
        part[n] = jnp.dot(hid[...], wd[n], preferred_element_type=F32).astype(BF16)
        send(part.at[n, pl.ds((1 - c) * half, half)], r1.at[n], s1s.at[n], r1s.at[n], partner)

    def sum_core(n):
        took(r1.at[n], r1s.at[n])
        mine = part[n, pl.ds(c * half, half), :].astype(F32) + r1[n].astype(F32)
        s1[n] = mine.astype(BF16)
        for d in range(1, cols):
            to = lax.rem(x + d, cols)
            send(s1.at[n, pl.ds(to * block, block)], r2.at[n, d - 1], s2s.at[n, d - 1], r2s.at[n], at_x(d))

    def sum_x(n):
        took(r2.at[n], r2s.at[n])
        mine = s1[n, pl.ds(x * block, block), :].astype(F32)
        for d in range(cols - 1):
            mine = mine + r2[n, d].astype(F32)
        for i in range(ep):
            b3[n, i] = mine[i * rows:(i + 1) * rows].astype(BF16)
        for d in range(1, ep):
            to = paired(e, d)
            send(b3.at[n, to], r3.at[n, d - 1], s3s.at[n, d - 1], r3s.at[n], at_z(d))

    def sum_z(n):
        took(r3.at[n], r3s.at[n])
        total = b3[n, e].astype(F32)
        for d in range(ep - 1):
            total = total + r3[n, d].astype(F32)
        out_ref[:, n * nw:(n + 1) * nw] = total.astype(BF16)

    for s in range(nc + LAG1 + LAG2 + LAG3):
        if s < nc:
            down(s)
        if 0 <= s - LAG1 < nc:
            sum_core(s - LAG1)
        if 0 <= s - LAG1 - LAG2 < nc:
            sum_x(s - LAG1 - LAG2)
        if 0 <= s - LAG1 - LAG2 - LAG3 < nc:
            sum_z(s - LAG1 - LAG2 - LAG3)
    for cp in sends:
        cp.wait_send()


def solution(mesh):
    ep, tok = mesh.shape["ep"], mesh.shape["tok"]
    cols = tok // 2

    def step(tokens, expert_ids, gate_fixed, w_gate, w_up, w_down):
        rows, width = tokens.shape
        ff = w_gate.shape[2]
        m = ep * tok * rows
        nk = chunks_of(width, NK)
        nc = chunks_of(width, NC)
        kc, nw = width // nk, width // nc
        dma = pltpu.SemaphoreType.DMA
        vmem = pl.BlockSpec(memory_space=pltpu.VMEM)
        anywhere = pl.BlockSpec(memory_space=pl.ANY)
        return pl.pallas_call(
            functools.partial(kernel, ep, cols, nk, nc),
            out_shape=jax.ShapeDtypeStruct((rows, width), BF16),
            in_specs=[anywhere, anywhere, anywhere, anywhere, anywhere, anywhere],
            out_specs=vmem,
            scratch_shapes=[
                pltpu.VMEM(expert_ids.shape[::-1], jnp.int32),
                pltpu.VMEM(gate_fixed.shape[::-1], jnp.int32),
                pltpu.VMEM((nk, kc, ff), BF16),
                pltpu.VMEM((nk, kc, ff), BF16),
                pltpu.VMEM((nc, ff, nw), BF16),
                pltpu.VMEM((nk, tok, ep, rows, kc), BF16),
                pltpu.VMEM((tok, ep, rows, 128), F32),
                pltpu.VMEM((m, kc), BF16),
                pltpu.VMEM((m, ff), F32),
                pltpu.VMEM((m, ff), F32),
                pltpu.VMEM((m, ff), BF16),
                pltpu.VMEM((nc, m, nw), BF16),
                pltpu.VMEM((nc, m // 2, nw), BF16),
                pltpu.VMEM((nc, m // 2, nw), BF16),
                pltpu.VMEM((nc, cols - 1, ep * rows, nw), BF16),
                pltpu.VMEM((nc, ep, rows, nw), BF16),
                pltpu.VMEM((nc, ep - 1, rows, nw), BF16),
                dma((2,)), dma((nk,)), dma((nk,)), dma((nc,)), dma((nk,)),
                dma((nk + 1, ep - 1)), dma((nk + 1, ep - 1)),
                dma((nk + 1, ep, cols - 1)), dma((nk + 1, cols - 1)),
                dma((nk + 1, cols)), dma((nk + 1,)),
                dma((nc,)), dma((nc,)),
                dma((nc, cols - 1)), dma((nc,)),
                dma((nc, ep - 1)), dma((nc,)),
            ],
            compiler_params=pltpu.CompilerParams(
                collective_id=0, has_side_effects=True, vmem_limit_bytes=64000000,
            ),
        )(expert_ids.T, gate_fixed.T, tokens, w_gate, w_up, w_down)

    rows_spec = P(("groups", "ep", "tok"), None)
    return jax.shard_map(
        step, mesh=mesh,
        in_specs=(rows_spec, rows_spec, rows_spec, P("ep", None, "tok"), P("ep", None, "tok"), P("ep", "tok", None)),
        out_specs=rows_spec, check_vma=False,
    )
```
